32 devices in a mesh: ctx: 16 (over z, x, core), tp: 2 (over y).
Axes of the slice: x: 2, y: 2, z: 4, core: 2. Of those that a mesh axis runs over, the one named last changes fastest.
Arguments:
- token_ids: int32 [12288], P('ctx'), may hold values from 0 to 511
- embed_table: bfloat16 [512, 4096], replicated, may hold values from -6 to 6
- norm_gain: float32 [4096], replicated, may hold values from 0.25 to 1.75
- w_in: bfloat16 [4096, 3, 2048], P(None, None, 'tp'), may hold values from -0.09375 to 0.09375
- short_taps: float32 [3, 3, 2048], P(None, None, 'tp'), may hold values from -3 to 3
- long_filter: bfloat16 [2048, 12288], P('tp', 'ctx'), may hold values from -0.0546875 to 0.0546875
- skip_gain: float32 [2048], P('tp'), may hold values from 0.5 to 2
- w_out: bfloat16 [2048, 4096], P(None, 'tp'), may hold values from -0.125 to 0.125
Outputs:
- mixed: bfloat16 [12288, 4096], P('ctx', 'tp')
The draws below stay inside these ranges and needn't reach their ends.
All inputs are finite; a program needn't handle non-finite values.
Results may differ from the reference program's by a relative error of at most 0.0095.
Values may be sent and summed in bfloat16 or wider, within the bound.
No kernel may reach another device: no remote copies, remote signals or barrier semaphores. Data moves between devices by JAX's collectives and lax.ppermute only.
A program may use at most 192 MiB of HBM per device.

```python
import math
import jax
import jax.numpy as jnp
import numpy as np
from jax import lax

D = 4096
C = 2048
V = 512
SEQ = 12288


def touch_ends(result, stream_key, smallest, largest):
    longest = result.shape.index(max(result.shape))
    spots = []
    for shift in (0, 1):
        where = [jax.random.randint(jax.random.fold_in(stream_key, axis), (), 0, length) for axis, length in enumerate(result.shape)]
        where[longest] = (where[longest] + shift) % result.shape[longest]
        spots.append(tuple(where))
    return result.at[spots[0]].set(smallest).at[spots[1]].set(largest)


def block_levels(stream_key, extent, split, least, largest):
    def one(axis_at, parts):
        draws = jax.random.uniform(jax.random.fold_in(jax.random.fold_in(stream_key, 6), axis_at), (parts,), jnp.float32, least / len(split), largest / len(split))
        return jnp.repeat(jnp.exp(draws), extent[axis_at] // parts).reshape((-1,) + (1,) * (len(extent) - axis_at - 1))

    factor_of = one(*split[0])
    for cut in split[1:]:
        factor_of = factor_of * one(*cut)
    return factor_of


def rank_bounds(amount, lean):
    weights = [(1 << 20) // math.isqrt(grade ** lean) + 1 for grade in range(1, amount + 1)]
    deviation = 1 + sum(weights) // (1 << 30)
    return np.cumsum(np.array([max(1, weight // deviation) for weight in weights]))


def skewed_ids(rng, shape, amount, lean):
    listing = rank_bounds(amount, lean)
    ticket = jax.random.randint(jax.random.fold_in(rng, 1), shape, 0, int(listing[amount - 1]))
    grade = jnp.searchsorted(jnp.asarray(listing, jnp.int32), ticket, side="right")
    return jax.random.permutation(jax.random.fold_in(rng, 2), amount)[grade].astype(jnp.int32)


def scatter_about(rng, dims, deviation, limit, cuts=(), dtype=jnp.bfloat16):
    drawn = deviation * jax.random.normal(rng, dims, jnp.float32)
    if cuts:
        drawn = drawn * block_levels(rng, dims, cuts, -0.22, 0.18)
    return jnp.clip(drawn, -limit, limit).astype(dtype)


def setup_inputs(seed: int = 0) -> dict:
    seeds = jax.random.split(jax.random.key(seed), 9)
    return {
        "token_ids": touch_ends(skewed_ids(seeds[0], (SEQ,), V, 2), jax.random.fold_in(seeds[0], 3), 0, V - 1).astype(jnp.int32),
        "embed_table": scatter_about(seeds[1], (V, D), 1.0, 6.0),
        "norm_gain": jnp.clip(1.0 + 0.15 * jax.random.normal(seeds[2], (D,), jnp.float32), 0.25, 1.75),
        "w_in": scatter_about(seeds[3], (D, 3, C), D ** -0.5, 0.09375, ((2, 2),)),
        "short_taps": scatter_about(seeds[4], (3, 3, C), 0.6, 3.0, ((2, 2),), jnp.float32),
        "long_filter": scatter_about(seeds[5], (C, SEQ), SEQ ** -0.5, 0.0546875, ((0, 2), (1, 16))),
        "skip_gain": jnp.clip(0.5 + 1.5 * jax.random.uniform(seeds[6], (C,), jnp.float32) ** block_levels(seeds[6], (C,), ((0, 2),), -0.2, 0.2), 0.5, 2.0),
        "w_out": scatter_about(seeds[7], (C, D), C ** -0.5, 0.125, ((1, 2),)),
    }


norm_eps = 1e-06

def causal_conv(pair):
    signal, kernel = pair
    length = signal.shape[-1]
    spectrum = jnp.fft.rfft(signal, n=2 * length, axis=-1) * jnp.fft.rfft(kernel, n=2 * length, axis=-1)
    return jnp.fft.irfft(spectrum, n=2 * length, axis=-1)[:, :length]

def reference(token_ids, embed_table, norm_gain, w_in, short_taps, long_filter, skip_gain, w_out):
    embedded = jnp.take(embed_table, token_ids, axis=0).astype(jnp.float32)
    scale = lax.rsqrt(lax.optimization_barrier(jnp.mean(embedded * embedded, axis=1, keepdims=True)) + norm_eps)
    normed = (embedded * scale * norm_gain).astype(jnp.bfloat16)
    width = normed.shape[1]
    channels = w_in.shape[2]
    projected = jnp.dot(normed.astype(jnp.float32), w_in.reshape(width, 3 * channels).astype(jnp.float32), precision=lax.Precision.HIGHEST, preferred_element_type=jnp.float32)
    projected = lax.optimization_barrier(projected.astype(jnp.bfloat16))
    projected = projected.reshape(-1, 3, channels).astype(jnp.float32)
    once = jnp.pad(projected, ((1, 0), (0, 0), (0, 0)))[:-1]
    twice = jnp.pad(projected, ((2, 0), (0, 0), (0, 0)))[:-2]
    shortened = short_taps[0] * projected + short_taps[1] * once + short_taps[2] * twice
    shortened = lax.optimization_barrier(shortened.astype(jnp.bfloat16)).astype(jnp.float32)
    query = shortened[:, 0, :].T
    key_side = shortened[:, 1, :]
    value_side = shortened[:, 2, :]
    product = lax.optimization_barrier((key_side * value_side).astype(jnp.bfloat16))
    product = product.astype(jnp.float32).T
    length = product.shape[1]
    filters = long_filter.astype(jnp.float32)
    block = 128
    convolved = lax.map(causal_conv, (product.reshape(channels // block, block, length), filters.reshape(channels // block, block, length)))
    convolved = convolved.reshape(channels, length)
    skipped = lax.optimization_barrier((convolved + skip_gain[:, None] * product).astype(jnp.bfloat16))
    gated = (query * skipped.astype(jnp.float32)).astype(jnp.bfloat16)
    gated_rows = gated.astype(jnp.float32).T
    projected_out = jnp.dot(gated_rows, w_out.astype(jnp.float32), precision=lax.Precision.HIGHEST, preferred_element_type=jnp.float32)
    return (embedded + projected_out).astype(jnp.bfloat16)
```

```python
import functools

import jax
import jax.numpy as jnp
import numpy as np
from jax import lax
from jax.experimental import pallas as pl
from jax.experimental.pallas import tpu as pltpu
from jax.sharding import PartitionSpec as P

norm_eps = 1e-06
COLS = 256
HALO = 128
CHUNKS = 2


def split_table(table):
    high = table.astype(jnp.bfloat16)
    low = (table - high.astype(np.float32)).astype(jnp.bfloat16)
    return high, low


def transform_tables(rows):
    period = 2 * rows
    total = period * COLS
    kept = -(-(rows + 1) // 16) * 16
    k1 = np.arange(kept)
    live = (k1 <= rows)[:, None]
    angle = 2 * np.pi * (k1[:, None] * np.arange(rows)[None] % period) / period
    first = np.concatenate([np.cos(angle) * live, -np.sin(angle) * live]).astype(np.float32)
    twist = 2 * np.pi * (k1[:, None] * np.arange(COLS)[None]) / total
    cos_twist, sin_twist = np.cos(twist).astype(np.float32), np.sin(twist).astype(np.float32)
    col = 2 * np.pi * (np.arange(COLS)[:, None] * np.arange(COLS)[None] % COLS) / COLS
    c, s = np.cos(col), np.sin(col)
    forward = np.block([[c, -s], [s, c]]).astype(jnp.bfloat16)
    backward = np.block([[c, s], [-s, c]]).astype(jnp.bfloat16)
    weight = np.where((k1 == 0) | (k1 == rows), 1.0, 2.0)[:, None] * live / total
    last = np.concatenate([np.cos(angle) * weight, -np.sin(angle) * weight]).T.astype(np.float32)
    first = np.concatenate(split_table(first), axis=1)
    last = np.concatenate(split_table(last), axis=1)
    return kept, (first, cos_twist, sin_twist, forward, backward, last)


def dot(left, right):
    return jnp.dot(left, right, preferred_element_type=jnp.float32)


def lookup_body(ids_ref, table_ref, taps_ref, query_ref, product_ref):
    ids = ids_ref[0]
    vocab = table_ref.shape[1]
    owned = query_ref.shape[0]
    rows = lax.broadcasted_iota(jnp.int32, (vocab, ids.shape[1]), 0)
    one_hot = jnp.where(rows == ids, 1.0, 0.0).astype(jnp.bfloat16)
    projected = dot(table_ref[...], one_hot)
    once = pltpu.roll(projected, 1, 1)
    twice = pltpu.roll(projected, 2, 1)
    short = (
        taps_ref[:, 0:1] * projected[:, HALO:]
        + taps_ref[:, 1:2] * once[:, HALO:]
        + taps_ref[:, 2:3] * twice[:, HALO:]
    ).astype(jnp.bfloat16)
    query_ref[...] = short[:owned]
    key_side = short[owned : 2 * owned].astype(jnp.float32)
    value_side = short[2 * owned :].astype(jnp.float32)
    product_ref[...] = (key_side * value_side).astype(jnp.bfloat16)


def lookup(ids, table, taps, steps):
    length = ids.shape[0]
    owned = table.shape[0] // 3
    block = length // steps
    padded = jnp.pad(ids, (HALO, 0), constant_values=-1)
    blocks = jnp.stack([padded[i * block : (i + 1) * block + HALO] for i in range(steps)])[:, None]
    out = jax.ShapeDtypeStruct((owned, length), jnp.bfloat16)
    spec = pl.BlockSpec((owned, block), lambda i: (0, i))
    return pl.pallas_call(
        lookup_body,
        grid=(steps,),
        in_specs=[
            pl.BlockSpec((1, 1, block + HALO), lambda i: (i, 0, 0)),
            pl.BlockSpec(table.shape, lambda i: (0, 0)),
            pl.BlockSpec(taps.shape, lambda i: (0, 0)),
        ],
        out_specs=[spec, spec],
        out_shape=[out, out],
        name="lookup",
    )(blocks, table, taps)


def conv_body(
    kept, x_ref, h_ref, q_ref, skip_ref, first_ref, cos_ref, sin_ref, fwd_ref, bwd_ref, last_ref,
    out_ref, turned, joint,
):
    group = x_ref.shape[0]
    cos, sin = cos_ref[...], sin_ref[...]
    half = group * kept
    for which, source in enumerate((x_ref, h_ref)):
        for c in range(group):
            block = source[c]
            stage = dot(first_ref[...], jnp.concatenate([block, block], axis=0))
            real, imag = stage[:kept], stage[kept:]
            at = pl.ds(which * half + c * kept, kept)
            turned[at, :COLS] = (real * cos + imag * sin).astype(jnp.bfloat16)
            turned[at, COLS:] = (imag * cos - real * sin).astype(jnp.bfloat16)
    spec_x = dot(turned[:half], fwd_ref[...])
    spec_h = dot(turned[half:], fwd_ref[...])
    xr, xi = spec_x[:, :COLS], spec_x[:, COLS:]
    hr, hi = spec_h[:, :COLS], spec_h[:, COLS:]
    joint[:, :COLS] = (xr * hr - xi * hi).astype(jnp.bfloat16)
    joint[:, COLS:] = (xr * hi + xi * hr).astype(jnp.bfloat16)
    back = dot(joint[...], bwd_ref[...])
    for c in range(group):
        real = back[c * kept : (c + 1) * kept, :COLS]
        imag = back[c * kept : (c + 1) * kept, COLS:]
        un_real = (real * cos - imag * sin).astype(jnp.bfloat16)
        un_imag = (imag * cos + real * sin).astype(jnp.bfloat16)
        convolved = dot(last_ref[...], jnp.concatenate([un_real, un_imag, un_real, un_imag], axis=0))
        skipped = (convolved + skip_ref[c] * x_ref[c].astype(jnp.float32)).astype(jnp.bfloat16)
        out_ref[c] = (q_ref[c].astype(jnp.float32) * skipped.astype(jnp.float32)).astype(jnp.bfloat16)


def gated_conv(product, kernel, query, skip):
    channels, rows, cols = product.shape
    kept, tables = transform_tables(rows)
    group = min(8, channels)
    spec = pl.BlockSpec((group, rows, cols), lambda i: (i, 0, 0))
    skip = jnp.broadcast_to(skip[:, None, None], (channels, 1, cols))
    return pl.pallas_call(
        functools.partial(conv_body, kept),
        grid=(channels // group,),
        in_specs=[spec, spec, spec, pl.BlockSpec((group, 1, cols), lambda i: (i, 0, 0))]
        + [pl.BlockSpec(t.shape, lambda i: (0, 0)) for t in tables],
        out_specs=spec,
        out_shape=jax.ShapeDtypeStruct(product.shape, jnp.bfloat16),
        scratch_shapes=[
            pltpu.VMEM((2 * group * kept, 2 * cols), jnp.bfloat16),
            pltpu.VMEM((group * kept, 2 * cols), jnp.bfloat16),
        ],
        name="gated_conv",
    )(product, kernel, query, skip, *[jnp.asarray(t) for t in tables])


def local(token_ids, embed_table, norm_gain, w_in, short_taps, long_filter, skip_gain, w_out):
    vocab, width = embed_table.shape
    groups = lax.axis_size("ctx")
    here = lax.axis_index("ctx")
    positions = token_ids.shape[0]
    chan_part = w_in.shape[2]
    part = chan_part // CHUNKS
    piece = part // groups
    owned = CHUNKS * piece
    length = groups * positions
    rows = length // COLS

    def own(array, axis):
        cuts = [
            lax.dynamic_slice_in_dim(array, k * part + here * piece, piece, axis)
            for k in range(CHUNKS)
        ]
        return jnp.concatenate(cuts, axis=axis)

    all_ids = lax.all_gather(token_ids, "ctx", axis=0, tiled=True)
    outgoing = long_filter.reshape(CHUNKS, groups, piece, positions).transpose(1, 0, 2, 3)
    arrived = lax.all_to_all(
        outgoing.reshape(groups, owned, positions), "ctx", split_axis=0, concat_axis=0, tiled=True
    )
    table32 = embed_table.astype(jnp.float32)
    scale = lax.rsqrt(jnp.mean(table32 * table32, axis=1, keepdims=True) + norm_eps)
    normed = (table32 * scale * norm_gain).astype(jnp.bfloat16)
    w_own = own(w_in, 2).reshape(width, 3 * owned)
    proj_table = lax.dot_general(
        w_own, normed, (((0,), (1,)), ((), ())), preferred_element_type=jnp.float32
    ).astype(jnp.bfloat16)
    taps = own(short_taps, 2).reshape(3, 3 * owned).T
    query, product = lookup(all_ids, proj_table, taps, groups // 2)
    query = query.reshape(owned, rows, COLS)
    product = product.reshape(owned, rows, COLS)
    kernel = arrived.transpose(1, 0, 2).reshape(owned, rows, COLS)
    skip = own(skip_gain, 0)

    width_part = w_out.shape[1]
    own_table = lax.dynamic_slice_in_dim(
        embed_table, lax.axis_index("tp") * width_part, width_part, 1
    )
    one_hot = (token_ids[:, None] == jnp.arange(vocab, dtype=jnp.int32)[None, :]).astype(
        jnp.bfloat16
    )
    total = dot(one_hot, own_table)
    out_rows = w_out.reshape(-1, CHUNKS, part, width_part)
    for k in range(CHUNKS):
        cut = slice(k * piece, (k + 1) * piece)
        gated = gated_conv(product[cut], kernel[cut], query[cut], skip[cut])
        gated = gated.reshape(piece, groups, positions).transpose(1, 0, 2)
        returned = lax.all_to_all(gated, "ctx", split_axis=0, concat_axis=0, tiled=True)
        gathered = lax.all_gather(returned.reshape(part, positions), "tp", axis=0)
        for j in range(gathered.shape[0]):
            total = total + lax.dot_general(
                gathered[j],
                out_rows[j, k],
                (((0,), (0,)), ((), ())),
                preferred_element_type=jnp.float32,
            )
    return total.astype(jnp.bfloat16)


def solution(mesh):
    return jax.shard_map(
        local,
        mesh=mesh,
        in_specs=(
            P("ctx"),
            P(),
            P(),
            P(None, None, "tp"),
            P(None, None, "tp"),
            P("tp", "ctx"),
            P("tp"),
            P(None, "tp"),
        ),
        out_specs=P("ctx", "tp"),
        check_vma=False,
    )
```

```python
import functools

import jax
import jax.numpy as jnp
import numpy as np
from jax import lax
from jax.experimental import pallas as pl
from jax.experimental.pallas import tpu as pltpu
from jax.sharding import PartitionSpec as P

norm_eps = 1e-06
COLS = 256
HALO = 128
CHUNKS = 2


def split_table(table):
    high = table.astype(jnp.bfloat16)
    low = (table - high.astype(np.float32)).astype(jnp.bfloat16)
    return high, low


def transform_tables(rows):
    period = 2 * rows
    total = period * COLS
    kept = -(-(rows + 1) // 16) * 16
    k1 = np.arange(kept)
    live = (k1 <= rows)[:, None]
    angle = 2 * np.pi * (k1[:, None] * np.arange(rows)[None] % period) / period
    first = np.concatenate([np.cos(angle) * live, -np.sin(angle) * live]).astype(np.float32)
    twist = 2 * np.pi * (k1[:, None] * np.arange(COLS)[None]) / total
    cos_twist, sin_twist = np.cos(twist).astype(np.float32), np.sin(twist).astype(np.float32)
    col = 2 * np.pi * (np.arange(COLS)[:, None] * np.arange(COLS)[None] % COLS) / COLS
    c, s = np.cos(col), np.sin(col)
    forward = np.block([[c, -s], [s, c]]).astype(jnp.bfloat16)
    backward = np.block([[c, s], [-s, c]]).astype(jnp.bfloat16)
    weight = np.where((k1 == 0) | (k1 == rows), 1.0, 2.0)[:, None] * live / total
    last = np.concatenate([np.cos(angle) * weight, -np.sin(angle) * weight]).T.astype(np.float32)
    first = np.concatenate(split_table(first), axis=1)
    last = np.concatenate(split_table(last), axis=1)
    return kept, (first, cos_twist, sin_twist, forward, backward, last)


def dot(left, right):
    return jnp.dot(left, right, preferred_element_type=jnp.float32)


def lookup_body(ids_ref, table_ref, taps_ref, query_ref, product_ref):
    ids = ids_ref[0]
    vocab = table_ref.shape[1]
    owned = query_ref.shape[0]
    rows = lax.broadcasted_iota(jnp.int32, (vocab, ids.shape[1]), 0)
    one_hot = jnp.where(rows == ids, 1.0, 0.0).astype(jnp.bfloat16)
    projected = dot(table_ref[...], one_hot)
    once = pltpu.roll(projected, 1, 1)
    twice = pltpu.roll(projected, 2, 1)
    short = (
        taps_ref[:, 0:1] * projected[:, HALO:]
        + taps_ref[:, 1:2] * once[:, HALO:]
        + taps_ref[:, 2:3] * twice[:, HALO:]
    ).astype(jnp.bfloat16)
    query_ref[...] = short[:owned]
    key_side = short[owned : 2 * owned].astype(jnp.float32)
    value_side = short[2 * owned :].astype(jnp.float32)
    product_ref[...] = (key_side * value_side).astype(jnp.bfloat16)


def lookup(ids, table, taps, steps):
    length = ids.shape[0]
    owned = table.shape[0] // 3
    block = length // steps
    padded = jnp.pad(ids, (HALO, 0), constant_values=-1)
    blocks = jnp.stack([padded[i * block : (i + 1) * block + HALO] for i in range(steps)])[:, None]
    out = jax.ShapeDtypeStruct((owned, length), jnp.bfloat16)
    spec = pl.BlockSpec((owned, block), lambda i: (0, i))
    return pl.pallas_call(
        lookup_body,
        grid=(steps,),
        in_specs=[
            pl.BlockSpec((1, 1, block + HALO), lambda i: (i, 0, 0)),
            pl.BlockSpec(table.shape, lambda i: (0, 0)),
            pl.BlockSpec(taps.shape, lambda i: (0, 0)),
        ],
        out_specs=[spec, spec],
        out_shape=[out, out],
        name="lookup",
    )(blocks, table, taps)


def conv_body(
    kept, x_ref, h_ref, q_ref, skip_ref, first_ref, cos_ref, sin_ref, fwd_ref, bwd_ref, last_ref,
    out_ref, turned, joint,
):
    group = x_ref.shape[0]
    cos, sin = cos_ref[...], sin_ref[...]
    half = group * kept
    for which, source in enumerate((x_ref, h_ref)):
        for c in range(group):
            block = source[c]
            stage = dot(first_ref[...], jnp.concatenate([block, block], axis=0))
            real, imag = stage[:kept], stage[kept:]
            at = pl.ds(which * half + c * kept, kept)
            turned[at, :COLS] = (real * cos + imag * sin).astype(jnp.bfloat16)
            turned[at, COLS:] = (imag * cos - real * sin).astype(jnp.bfloat16)
    spec_x = dot(turned[:half], fwd_ref[...])
    spec_h = dot(turned[half:], fwd_ref[...])
    xr, xi = spec_x[:, :COLS], spec_x[:, COLS:]
    hr, hi = spec_h[:, :COLS], spec_h[:, COLS:]
    joint[:, :COLS] = (xr * hr - xi * hi).astype(jnp.bfloat16)
    joint[:, COLS:] = (xr * hi + xi * hr).astype(jnp.bfloat16)
    back = dot(joint[...], bwd_ref[...])
    for c in range(group):
        real = back[c * kept : (c + 1) * kept, :COLS]
        imag = back[c * kept : (c + 1) * kept, COLS:]
        un_real = (real * cos - imag * sin).astype(jnp.bfloat16)
        un_imag = (imag * cos + real * sin).astype(jnp.bfloat16)
        convolved = dot(last_ref[...], jnp.concatenate([un_real, un_imag, un_real, un_imag], axis=0))
        skipped = (convolved + skip_ref[c] * x_ref[c].astype(jnp.float32)).astype(jnp.bfloat16)
        out_ref[c] = (q_ref[c].astype(jnp.float32) * skipped.astype(jnp.float32)).astype(jnp.bfloat16)


def gated_conv(product, kernel, query, skip, start, channels):
    rows, cols = product.shape[1:]
    kept, tables = transform_tables(rows)
    group = min(8, channels)
    offset = start // group
    spec = pl.BlockSpec((group, rows, cols), lambda i: (i + offset, 0, 0))
    return pl.pallas_call(
        functools.partial(conv_body, kept),
        grid=(channels // group,),
        in_specs=[spec, spec, spec, pl.BlockSpec((group, 1, cols), lambda i: (i + offset, 0, 0))]
        + [pl.BlockSpec(t.shape, lambda i: (0, 0)) for t in tables],
        out_specs=pl.BlockSpec((group, rows, cols), lambda i: (i, 0, 0)),
        out_shape=jax.ShapeDtypeStruct((channels, rows, cols), jnp.bfloat16),
        scratch_shapes=[
            pltpu.VMEM((2 * group * kept, 2 * cols), jnp.bfloat16),
            pltpu.VMEM((group * kept, 2 * cols), jnp.bfloat16),
        ],
        name="gated_conv",
    )(product, kernel, query, skip, *[jnp.asarray(t) for t in tables])


def local(token_ids, embed_table, norm_gain, w_in, short_taps, long_filter, skip_gain, w_out):
    vocab, width = embed_table.shape
    groups = lax.axis_size("ctx")
    here = lax.axis_index("ctx")
    positions = token_ids.shape[0]
    chan_part = w_in.shape[2]
    part = chan_part // CHUNKS
    piece = part // groups
    owned = CHUNKS * piece
    length = groups * positions
    rows = length // COLS

    def own(array, axis):
        cuts = [
            lax.dynamic_slice_in_dim(array, k * part + here * piece, piece, axis)
            for k in range(CHUNKS)
        ]
        return jnp.concatenate(cuts, axis=axis)

    all_ids = lax.all_gather(token_ids, "ctx", axis=0, tiled=True)
    all_ids, long_filter = lax.optimization_barrier((all_ids, long_filter))
    outgoing = long_filter.reshape(CHUNKS, groups, piece, positions).transpose(1, 0, 2, 3)
    arrived = lax.all_to_all(
        outgoing.reshape(groups, owned, positions), "ctx", split_axis=0, concat_axis=0, tiled=True
    )
    table32 = embed_table.astype(jnp.float32)
    scale = lax.rsqrt(jnp.mean(table32 * table32, axis=1, keepdims=True) + norm_eps)
    normed = (table32 * scale * norm_gain).astype(jnp.bfloat16)
    w_own = own(w_in, 2).reshape(width, 3 * owned)
    proj_table = lax.dot_general(
        w_own, normed, (((0,), (1,)), ((), ())), preferred_element_type=jnp.float32
    ).astype(jnp.bfloat16)
    taps = own(short_taps, 2).reshape(3, 3 * owned).T
    query, product = lookup(all_ids, proj_table, taps, groups // 2)
    query = query.reshape(owned, rows, COLS)
    product = product.reshape(owned, rows, COLS)
    kernel = arrived.transpose(1, 0, 2).reshape(owned, rows, COLS)
    skip = jnp.broadcast_to(own(skip_gain, 0)[:, None, None], (owned, 1, COLS))

    width_part = w_out.shape[1]
    sides = lax.axis_size("tp")
    side = lax.axis_index("tp")
    own_table = lax.dynamic_slice_in_dim(embed_table, side * width_part, width_part, 1)
    one_hot = (token_ids[:, None] == jnp.arange(vocab, dtype=jnp.int32)[None, :]).astype(
        jnp.bfloat16
    )
    total = dot(one_hot, own_table)
    out_rows = w_out.reshape(sides * CHUNKS, part, width_part)

    def add_side(total, block, origin, k):
        weights = lax.dynamic_index_in_dim(out_rows, origin * CHUNKS + k, 0, keepdims=False)
        return total + lax.dot_general(
            block, weights, (((0,), (0,)), ((), ())), preferred_element_type=jnp.float32
        )

    for k in range(CHUNKS):
        gated = gated_conv(product, kernel, query, skip, k * piece, piece)
        gated = gated.reshape(piece, groups, positions).transpose(1, 0, 2)
        returned = lax.all_to_all(gated, "ctx", split_axis=0, concat_axis=0, tiled=True)
        returned = returned.reshape(part, positions)
        others = [
            lax.ppermute(returned, "tp", [(i, (i + hop) % sides) for i in range(sides)])
            for hop in range(1, sides)
        ]
        total = add_side(total, returned, side, k)
        for hop, block in enumerate(others, 1):
            total = add_side(total, block, (side - hop) % sides, k)
    return total.astype(jnp.bfloat16)


def solution(mesh):
    return jax.shard_map(
        local,
        mesh=mesh,
        in_specs=(
            P("ctx"),
            P(),
            P(),
            P(None, None, "tp"),
            P(None, None, "tp"),
            P("tp", "ctx"),
            P("tp"),
            P(None, "tp"),
        ),
        out_specs=P("ctx", "tp"),
        check_vma=False,
    )
```
